32 devices in a mesh: tok: 4 (over x, core), col: 8 (over z, y).
Axes of the slice: x: 2, y: 2, z: 4, core: 2. Of those that a mesh axis runs over, the one named last changes fastest.
Arguments:
- hidden_in: bfloat16 [1024, 36864], P('tok', 'col'), may hold values from -6 to 6
- down_weight: bfloat16 [4608, 36864], P('col', 'tok'), may hold values from -0.046875 to 0.046875
- keep_mask: int32 [4608, 36864], P('col', 'tok'), may hold values 0 or 1
Outputs:
- layer_out: bfloat16 [1024, 4608], P(('tok', 'col'))
- hessian: float32 [4608, 4608], P('col', 'tok')
The draws below stay inside these ranges and needn't reach their ends.
All inputs are finite; a program needn't handle non-finite values. No bound on the sum of `keep_mask` on one device may be relied on, other than what follows from the above.
Results may differ from the reference program's by a relative error of at most 0.012.
Values may be sent and summed in bfloat16 or wider, within the bound.
No kernel may reach another device: no remote copies, remote signals or barrier semaphores. Data moves between devices by JAX's collectives and lax.ppermute only.
A program may use at most 192 MiB of HBM per device.

```python
import jax
import jax.numpy as jnp
from jax import lax

D = 4608
FF = 36864
TOKENS = 1024


def touch_ends(array, stream_key, least, top_value):
    extent = array.shape
    index_at = [jax.random.randint(jax.random.fold_in(stream_key, axis), (), 0, extent[axis]) for axis in range(len(extent))]
    array = array.at[tuple(index_at)].set(least)
    longest = extent.index(max(extent))
    index_at[longest] = (index_at[longest] + 1) % extent[longest]
    return array.at[tuple(index_at)].set(top_value)


def block_scale(rng, shape, cuts, least, largest):
    factor_of, own = 1.0, jax.random.fold_in(rng, 6)
    for axis_at, blocks in cuts:
        heights = jnp.exp(jax.random.uniform(jax.random.fold_in(own, axis_at), (blocks,), jnp.float32, least / len(cuts), largest / len(cuts)))
        factor_of = factor_of * jnp.repeat(heights, shape[axis_at] // blocks).reshape([-1 if axis == axis_at else 1 for axis in range(len(shape))])
    return factor_of


def scatter_about(stream_key, dims, spread, limit, shards=(), held_as=jnp.bfloat16):
    result = spread * jax.random.normal(stream_key, dims, jnp.float32)
    if shards:
        result = result * block_scale(stream_key, dims, shards, -0.22, 0.18)
    return jnp.clip(result, -limit, limit).astype(held_as)


def setup_inputs(seed: int = 0) -> dict:
    arg_keys = jax.random.split(jax.random.key(seed), 4)
    return {
        "hidden_in": scatter_about(arg_keys[0], (TOKENS, FF), 1.0, 6.0, ((0, 4), (1, 8))),
        "down_weight": scatter_about(arg_keys[1], (D, FF), (FF // 2) ** -0.5, 0.046875, ((0, 8), (1, 4))),
        "keep_mask": touch_ends((jax.random.randint(arg_keys[2], (D, FF), 0, 2) < 1).astype(jnp.int32), jax.random.fold_in(arg_keys[2], 1), 0, 1),
    }


def reference(hidden_in, down_weight, keep_mask):
    pruned = down_weight * keep_mask.astype(down_weight.dtype)
    layer_out = lax.dot_general(hidden_in, pruned, (((1,), (1,)), ((), ())), preferred_element_type=jnp.float32).astype(jnp.bfloat16)
    hessian = jnp.dot(layer_out.T, layer_out, preferred_element_type=jnp.float32) * (2.0 / TOKENS)
    return layer_out, hessian
```

```python
import jax
import jax.numpy as jnp
from jax import lax
from jax.sharding import Mesh, PartitionSpec as P

CHUNKS = 4
GROUPS = ((0, 1), (2, 3))


def swap(value, axis, offset):
    size = lax.axis_size(axis)
    return lax.ppermute(value, axis, [(i, i ^ offset) for i in range(size)])


def spread(value, axis):
    size = lax.axis_size(axis)
    if size != 4:
        return [value] + [swap(value, axis, k) for k in range(1, size)]
    near = swap(value, axis, 1)
    far = swap(value, axis, 2)
    middle = lax.ppermute(value, axis, [(1, 2), (2, 1)])
    ends = lax.ppermute(far, axis, [(1, 0), (2, 3)])
    index = lax.axis_index(axis)
    at_end = (index == 0) | (index == size - 1)
    return [value, near, far, lax.select(jnp.broadcast_to(at_end, value.shape), ends, middle)]


def xor_order(blocks, by):
    size = len(blocks)
    bit = 1
    while bit < size:
        flip = jnp.broadcast_to((by & bit) != 0, blocks[0].shape)
        blocks = [lax.select(flip, blocks[k ^ bit], blocks[k]) for k in range(size)]
        bit *= 2
    return blocks


def turn(blocks, axis):
    return blocks[:1] + [swap(blocks[k], axis, k) for k in range(1, len(blocks))]


def contract_last(left, right):
    return lax.dot_general(left, right, (((1,), (1,)), ((), ())), preferred_element_type=jnp.float32)


def contract_rows(left, right):
    return lax.dot_general(left, right, (((0,), (0,)), ((), ())), preferred_element_type=jnp.float32)


def body(hidden_in, down_weight, keep_mask):
    tok, row, sub = lax.axis_index("tok"), lax.axis_index("row"), lax.axis_index("sub")
    toks, subs = lax.axis_size("tok"), lax.axis_size("sub")
    rows, depth = hidden_in.shape
    cols = down_weight.shape[0]
    small = jnp.bfloat16

    def pruned(block):
        w = lax.dynamic_slice(down_weight, (0, block * depth), (cols, depth))
        return w * lax.dynamic_slice(keep_mask, (0, block * depth), (cols, depth)).astype(w.dtype)

    weights = [pruned(sub ^ k) for k in range(1, subs)]
    weights = [pruned(sub)] + [swap(w, "sub", k + 1) for k, w in enumerate(weights)]

    step = rows // CHUNKS
    shares = [[] for _ in range(subs)]
    for j in range(CHUNKS):
        seen = spread(hidden_in[j * step : (j + 1) * step], "row")
        mine = turn(xor_order(seen, tok ^ row), "tok")
        chunk = jnp.concatenate(mine, axis=0)
        for k in range(subs):
            shares[k].append(contract_last(chunk, weights[k]))

    left, right, layer_rows = [], [], []
    for group in GROUPS:
        n = len(group) * step

        def take(k):
            parts = [shares[k][j].reshape(toks, step, cols) for j in group]
            return jnp.concatenate(parts, axis=1) if len(parts) > 1 else parts[0]

        total = take(0)
        for k in range(1, subs):
            total = total + swap(take(k).astype(small), "sub", k).astype(jnp.float32)
        rest = total[1:].astype(small)
        layer = total[0]
        for k in range(1, toks):
            layer = layer + swap(rest[k - 1], "tok", k).astype(jnp.float32)
        layer = layer.astype(small)
        left.append(jnp.concatenate([layer] + [swap(layer, "tok", k) for k in range(1, toks)], axis=0))
        seen = spread(layer, "row")
        layer_rows.append(seen)
        mine = jnp.concatenate(turn(xor_order(seen, tok ^ row), "tok"), axis=0)
        both = [mine] + [swap(mine, "sub", k) for k in range(1, subs)]
        right.append(jnp.concatenate(xor_order(both, sub), axis=1))

    scaling = 2.0 / (rows * toks)
    hessian = contract_rows(jnp.concatenate(left, axis=0), jnp.concatenate(right, axis=0)) * scaling

    share = rows // (toks * subs)
    whole = [jnp.concatenate([g[k] for g in layer_rows], axis=0) if len(GROUPS) > 1 else layer_rows[0][k] for k in range(toks)]
    whole = jnp.stack(xor_order(whole, row), axis=0).reshape(toks, toks, subs, share, cols)

    def for_sub(other):
        return lax.dynamic_slice(whole, (0, row, other, 0, 0), (toks, 1, 1, share, cols)).reshape(toks, share, cols)

    pieces = [for_sub(sub)] + [swap(for_sub(sub ^ k), "sub", k) for k in range(1, subs)]
    layer_out = jnp.stack(xor_order(pieces, sub), axis=1).transpose(2, 0, 1, 3).reshape(share, toks * subs * cols)
    return layer_out, hessian


def solution(mesh):
    toks, both = mesh.shape["tok"], mesh.shape["col"]
    grid = Mesh(mesh.devices.reshape(toks, toks, both // toks), ("tok", "row", "sub"))
    col = ("row", "sub")
    in_specs = (P("tok", col), P(col, "tok"), P(col, "tok"))
    out_specs = (P(("tok",) + col, None), P(col, "tok"))
    return jax.shard_map(body, mesh=grid, in_specs=in_specs, out_specs=out_specs, check_vma=False)
```

```python
import functools

import jax
import jax.numpy as jnp
from jax import lax
from jax.experimental import pallas as pl
from jax.experimental.pallas import tpu as pltpu
from jax.sharding import Mesh, PartitionSpec as P


SHARES = (4, 4, 4, 2, 2)
GROUPS = ((0, 1, 2), (3, 4))


def swap(value, axis, offset):
    return lax.ppermute(value, axis, [(i, i ^ offset) for i in range(lax.axis_size(axis))])


def spread_first(value, axis):
    size = lax.axis_size(axis)
    if size != 4:
        return [value] + [swap(value, axis, k) for k in range(1, size)]
    near, far = swap(value, axis, 1), swap(value, axis, 2)
    return [value, near, far, lax.ppermute(value, axis, [(1, 2), (2, 1)])]


def spread_last(blocks, axis):
    if lax.axis_size(axis) != 4:
        return blocks
    return list(blocks) + [lax.ppermute(blocks[2], axis, [(1, 0), (2, 3)])]


def spread(value, axis):
    return spread_last(spread_first(value, axis), axis)


def order_kernel(size, by_ref, *refs):
    outs = refs[len(refs) - size :]
    blocks = refs[: len(refs) - size]

    def write(by, last):
        for k in range(size):
            at = k ^ by
            outs[k][...] = blocks[last if at == size - 1 else at][...]

    for by in range(size):
        if len(blocks) == size:
            pl.when(by_ref[0] == by)(functools.partial(write, by, size - 1))
        else:
            for end in range(2):
                pl.when((by_ref[0] == by) & (by_ref[1] == end))(functools.partial(write, by, size - 1 + end))


def xor_order(blocks, by, axis):
    size, index = lax.axis_size(axis), lax.axis_index(axis)
    at_end = (index == 0) | (index == size - 1)
    rows, cols = blocks[0].shape
    tile = 16 if rows % 16 == 0 and cols >= 2048 else rows
    spec = pl.BlockSpec((tile, cols), lambda i, by: (i, 0))
    return pl.pallas_call(
        functools.partial(order_kernel, size),
        grid_spec=pltpu.PrefetchScalarGridSpec(
            num_scalar_prefetch=1, grid=(rows // tile,), in_specs=[spec] * len(blocks), out_specs=[spec] * size
        ),
        out_shape=[jax.ShapeDtypeStruct((rows, cols), blocks[0].dtype)] * size,
        cost_estimate=pl.CostEstimate(flops=rows * cols * size, bytes_accessed=4 * rows * cols * size, transcendentals=0),
    )(jnp.stack([by, at_end.astype(jnp.int32)]), *blocks)


def turn(blocks, axis):
    return list(blocks[:1]) + [swap(blocks[k], axis, k) for k in range(1, len(blocks))]


def contract_last(left, right):
    return lax.dot_general(left, right, (((1,), (1,)), ((), ())), preferred_element_type=jnp.float32)


def contract_rows(left, right):
    return lax.dot_general(left, right, (((0,), (0,)), ((), ())), preferred_element_type=jnp.float32)


def body(hidden_in, down_weight, keep_mask):
    tok, row, sub = lax.axis_index("tok"), lax.axis_index("row"), lax.axis_index("sub")
    toks, subs = lax.axis_size("tok"), lax.axis_size("sub")
    rows, depth = hidden_in.shape
    cols = down_weight.shape[0]
    small = jnp.bfloat16
    steps = [rows * share // sum(SHARES) for share in SHARES]
    starts = [sum(steps[:j]) for j in range(len(steps))]

    def pruned(weight, mask, block):
        w = lax.dynamic_slice(weight, (0, block * depth), (cols, depth))
        return w * lax.dynamic_slice(mask, (0, block * depth), (cols, depth)).astype(w.dtype)

    pieces = lax.optimization_barrier([hidden_in[at : at + n] for at, n in zip(starts, steps)])
    seen = [spread_first(piece, "row") for piece in pieces]

    sent = [swap(pruned(down_weight, keep_mask, sub ^ k), "sub", k) for k in range(1, subs)]
    weight, mask, _ = lax.optimization_barrier((down_weight, keep_mask, seen[0][1]))
    weights = [pruned(weight, mask, sub)] + sent

    shares = [[] for _ in range(subs)]
    for j in range(len(steps)):
        blocks = spread_last(seen[j], "row")
        chunk = jnp.concatenate(turn(xor_order(blocks, tok ^ row, "row"), "tok"), axis=0)
        for k in range(subs):
            shares[k].append(contract_last(chunk, weights[k]))

    left, right, layer_rows = [], [], []
    for group in GROUPS:

        def take(k):
            parts = [shares[k][j].reshape(toks, steps[j], cols) for j in group]
            return jnp.concatenate(parts, axis=1) if len(parts) > 1 else parts[0]

        total = take(0)
        for k in range(1, subs):
            total = total + swap(take(k).astype(small), "sub", k).astype(jnp.float32)
        rest = total[1:].astype(small)
        layer = total[0]
        for k in range(1, toks):
            layer = layer + swap(rest[k - 1], "tok", k).astype(jnp.float32)
        layer = layer.astype(small)
        blocks = spread(layer, "row")
        left.append(jnp.concatenate(turn([layer] * toks, "tok"), axis=0))
        layer_rows.append(blocks)
        mine = jnp.concatenate(turn(xor_order(blocks, tok ^ row, "row"), "tok"), axis=0)
        both = [mine] + [swap(mine, "sub", k) for k in range(1, subs)]
        right.append(jnp.concatenate(xor_order(both, sub, "sub"), axis=1))

    scaling = 2.0 / (rows * toks)
    hessian = contract_rows(jnp.concatenate(left, axis=0), jnp.concatenate(right, axis=0)) * scaling

    share = rows // (toks * subs)
    whole = [jnp.concatenate(blocks, axis=0) for blocks in zip(*layer_rows)]
    whole = jnp.stack(xor_order(whole, row, "row"), axis=0).reshape(toks, toks, subs, share, cols)

    def for_sub(other):
        return lax.dynamic_slice(whole, (0, row, other, 0, 0), (toks, 1, 1, share, cols)).reshape(toks * share, cols)

    pieces = [for_sub(sub)] + [swap(for_sub(sub ^ k), "sub", k) for k in range(1, subs)]
    pieces = [piece.reshape(toks, share, cols) for piece in xor_order(pieces, sub, "sub")]
    layer_out = jnp.stack(pieces, axis=1).transpose(2, 0, 1, 3).reshape(share, toks * subs * cols)
    return layer_out, hessian


def solution(mesh):
    toks, both = mesh.shape["tok"], mesh.shape["col"]
    subs = both // toks
    grid = Mesh(mesh.devices.reshape(toks, toks, subs), ("tok", "row", "sub"))
    col = ("row", "sub")
    in_specs = (P("tok", col), P(col, "tok"), P(col, "tok"))
    out_specs = (P(("tok",) + col, None), P(col, "tok"))
    return jax.shard_map(body, mesh=grid, in_specs=in_specs, out_specs=out_specs, check_vma=False)
```

```python
import functools

import jax
import jax.numpy as jnp
from jax import lax
from jax.experimental import pallas as pl
from jax.experimental.pallas import tpu as pltpu
from jax.sharding import Mesh, PartitionSpec as P


SHARES = (4, 4, 4, 2, 2)
GROUPS = ((0, 1, 2), (3, 4))


def swap(value, axis, offset):
    return lax.ppermute(value, axis, [(i, i ^ offset) for i in range(lax.axis_size(axis))])


def spread_first(value, axis):
    size = lax.axis_size(axis)
    if size != 4:
        return [value] + [swap(value, axis, k) for k in range(1, size)]
    near, far = swap(value, axis, 1), swap(value, axis, 2)
    return [value, near, far, lax.ppermute(value, axis, [(1, 2), (2, 1)])]


def spread_last(blocks, axis):
    if lax.axis_size(axis) != 4:
        return blocks
    return list(blocks) + [lax.ppermute(blocks[2], axis, [(1, 0), (2, 3)])]


def spread(value, axis):
    return spread_last(spread_first(value, axis), axis)


def order_kernel(size, by_ref, *refs):
    outs, (held, in_sems, out_sems) = refs[-size - 3 : -3], refs[-3:]
    blocks = refs[: -size - 3]
    for k in range(size):
        at = k ^ by_ref[0]
        at = jnp.where((at == size - 1) & (by_ref[1] == 1), len(blocks) - 1, at)
        for b, block in enumerate(blocks):
            pl.when(at == b)(pltpu.make_async_copy(block, held.at[k], in_sems.at[k]).start)
    for k in range(size):
        pltpu.make_async_copy(blocks[0], held.at[k], in_sems.at[k]).wait()
        pltpu.make_async_copy(held.at[k], outs[k], out_sems.at[k]).start()
    for k in range(size):
        pltpu.make_async_copy(held.at[k], outs[k], out_sems.at[k]).wait()


def xor_order(blocks, by, axis):
    size, index = lax.axis_size(axis), lax.axis_index(axis)
    at_end = (index == 0) | (index == size - 1)
    rows, cols = blocks[0].shape
    dtype = blocks[0].dtype
    hbm = pl.BlockSpec(memory_space=pltpu.HBM)
    return pl.pallas_call(
        functools.partial(order_kernel, size),
        in_specs=[pl.BlockSpec(memory_space=pltpu.SMEM)] + [hbm] * len(blocks),
        out_specs=[hbm] * size,
        out_shape=[jax.ShapeDtypeStruct((rows, cols), dtype)] * size,
        scratch_shapes=[pltpu.VMEM((size, rows, cols), dtype), pltpu.SemaphoreType.DMA((size,)), pltpu.SemaphoreType.DMA((size,))],
        cost_estimate=pl.CostEstimate(flops=rows * cols * size, bytes_accessed=4 * rows * cols * size, transcendentals=0),
        name="order",
    )(jnp.stack([by, at_end.astype(jnp.int32)]), *blocks)


def product_kernel(toks, subs, chunks, *refs):
    lefts, weights = refs[: toks * chunks], refs[toks * chunks : toks * chunks + subs]
    keep, send, total = refs[toks * chunks + subs :]
    step = pl.program_id(0)
    left = jnp.concatenate([ref[...] for ref in lefts], axis=0)
    n = left.shape[0] // toks
    for k in range(subs):
        term = contract_last(left, weights[k][...])

        @pl.when(step == 0)
        def _(k=k, term=term):
            total[k] = term

        @pl.when(step > 0)
        def _(k=k, term=term):
            total[k] += term

    @pl.when(step == pl.num_programs(0) - 1)
    def _():
        for k in range(subs):
            for d in range(0, toks, 2):
                keep[k, d // 2] = total[k, d * n : (d + 1) * n]
                send[k, d // 2] = total[k, (d + 1) * n : (d + 2) * n].astype(send.dtype)


def product(lefts, weights):
    toks, chunks, subs = len(lefts), len(lefts[0]), len(weights)
    n = sum(piece.shape[0] for piece in lefts[0])
    cols, depth = weights[0].shape
    tile = depth // 4 if depth % 512 == 0 else depth
    flat = [piece for pieces in lefts for piece in pieces]
    shape = (subs, toks // 2, n, cols)
    whole = pl.BlockSpec(shape, lambda i: (0, 0, 0, 0))
    return pl.pallas_call(
        functools.partial(product_kernel, toks, subs, chunks),
        grid=(depth // tile,),
        in_specs=[pl.BlockSpec((piece.shape[0], tile), lambda i: (0, i)) for piece in flat]
        + [pl.BlockSpec((cols, tile), lambda i: (0, i))] * subs,
        out_specs=[whole, whole],
        out_shape=[jax.ShapeDtypeStruct(shape, jnp.float32), jax.ShapeDtypeStruct(shape, jnp.bfloat16)],
        scratch_shapes=[pltpu.VMEM((subs, toks * n, cols), jnp.float32)],
        cost_estimate=pl.CostEstimate(
            flops=2 * toks * n * cols * depth * subs, bytes_accessed=2 * depth * (toks * n + cols * subs), transcendentals=0
        ),
        name="product",
    )(*flat, *weights)


def select_order(blocks, by):
    size = len(blocks)
    bit = 1
    while bit < size:
        flip = jnp.broadcast_to((by & bit) != 0, blocks[0].shape)
        blocks = [lax.select(flip, blocks[k ^ bit], blocks[k]) for k in range(size)]
        bit *= 2
    return blocks


def turn(blocks, axis):
    return list(blocks[:1]) + [swap(blocks[k], axis, k) for k in range(1, len(blocks))]


def contract_last(left, right):
    return lax.dot_general(left, right, (((1,), (1,)), ((), ())), preferred_element_type=jnp.float32)


def contract_rows(left, right):
    return lax.dot_general(left, right, (((0,), (0,)), ((), ())), preferred_element_type=jnp.float32)


def body(hidden_in, down_weight, keep_mask):
    tok, row, sub = lax.axis_index("tok"), lax.axis_index("row"), lax.axis_index("sub")
    toks, subs = lax.axis_size("tok"), lax.axis_size("sub")
    rows, depth = hidden_in.shape
    cols = down_weight.shape[0]
    small = jnp.bfloat16
    steps = [rows * share // sum(SHARES) for share in SHARES]
    starts = [sum(steps[:j]) for j in range(len(steps))]

    def pruned(weight, mask, block):
        w = lax.dynamic_slice(weight, (0, block * depth), (cols, depth))
        return w * lax.dynamic_slice(mask, (0, block * depth), (cols, depth)).astype(w.dtype)

    pieces = lax.optimization_barrier([hidden_in[at : at + n] for at, n in zip(starts, steps)])
    seen = [spread_first(piece, "row") for piece in pieces]

    sent = [swap(pruned(down_weight, keep_mask, sub ^ k), "sub", k) for k in range(1, subs)]
    weight, mask, _ = lax.optimization_barrier((down_weight, keep_mask, seen[0][1]))
    weights = [pruned(weight, mask, sub)] + sent

    arrived = []
    for j in range(len(steps)):
        blocks = spread_last(seen[j], "row")
        arrived.append(turn(xor_order(blocks, tok ^ row, "row"), "tok"))

    left, right, layer_rows = [], [], []
    for group in GROUPS:
        keep, send = product([[arrived[j][d] for j in group] for d in range(toks)], weights)
        total = keep + swap(send, "tok", 1).astype(jnp.float32)
        rest = total[1:].astype(small)
        total = total[0]
        for k in range(1, subs):
            total = total + swap(rest[k - 1], "sub", k).astype(jnp.float32)
        bit = 2
        while bit < toks:
            total = total.reshape((-1, 2) + total.shape[1:])
            total = total[:, 0] + swap(total[:, 1].astype(small), "tok", bit).astype(jnp.float32)
            bit *= 2
        layer = total[0].astype(small)
        blocks = spread(layer, "row")
        left.append(jnp.concatenate(turn([layer] * toks, "tok"), axis=0))
        layer_rows.append(blocks)
        mine = jnp.concatenate(turn(xor_order(blocks, tok ^ row, "row"), "tok"), axis=0)
        both = [mine] + [swap(mine, "sub", k) for k in range(1, subs)]
        right.append(jnp.concatenate(select_order(both, sub), axis=1))

    scaling = 2.0 / (rows * toks)
    hessian = contract_rows(jnp.concatenate(left, axis=0), jnp.concatenate(right, axis=0)) * scaling

    share = rows // (toks * subs)
    whole = [jnp.concatenate(blocks, axis=0) for blocks in zip(*layer_rows)]
    whole = jnp.stack(xor_order(whole, row, "row"), axis=0).reshape(toks, toks, subs, share, cols)

    def for_sub(other):
        return lax.dynamic_slice(whole, (0, row, other, 0, 0), (toks, 1, 1, share, cols)).reshape(toks * share, cols)

    pieces = [for_sub(sub)] + [swap(for_sub(sub ^ k), "sub", k) for k in range(1, subs)]
    pieces = [piece.reshape(toks, share, cols) for piece in select_order(pieces, sub)]
    layer_out = jnp.stack(pieces, axis=1).transpose(2, 0, 1, 3).reshape(share, toks * subs * cols)
    return layer_out, hessian


def solution(mesh):
    toks, both = mesh.shape["tok"], mesh.shape["col"]
    subs = both // toks
    grid = Mesh(mesh.devices.reshape(toks, toks, subs), ("tok", "row", "sub"))
    col = ("row", "sub")
    in_specs = (P("tok", col), P(col, "tok"), P(col, "tok"))
    out_specs = (P(("tok",) + col, None), P(col, "tok"))
    return jax.shard_map(body, mesh=grid, in_specs=in_specs, out_specs=out_specs, check_vma=False)
```

```python
import functools

import jax
import jax.numpy as jnp
from jax import lax
from jax.experimental import pallas as pl
from jax.experimental.pallas import tpu as pltpu
from jax.sharding import Mesh, PartitionSpec as P


SHARES = (5, 4, 3, 2, 2)
GROUPS = ((0, 1, 2), (3, 4))


def swap(value, axis, offset):
    return lax.ppermute(value, axis, [(i, i ^ offset) for i in range(lax.axis_size(axis))])


def spread_first(value, axis):
    size = lax.axis_size(axis)
    if size != 4:
        return [value] + [swap(value, axis, k) for k in range(1, size)]
    near, far = swap(value, axis, 1), swap(value, axis, 2)
    return [value, near, far, lax.ppermute(value, axis, [(1, 2), (2, 1)])]


def spread_last(blocks, axis):
    if lax.axis_size(axis) != 4:
        return blocks
    return list(blocks) + [lax.ppermute(blocks[2], axis, [(1, 0), (2, 3)])]


def spread(value, axis):
    return spread_last(spread_first(value, axis), axis)


def order_kernel(size, by_ref, *refs):
    outs, (held, in_sems, out_sems) = refs[-size - 3 : -3], refs[-3:]
    blocks = refs[: -size - 3]
    for k in range(size):
        at = k ^ by_ref[0]
        at = jnp.where((at == size - 1) & (by_ref[1] == 1), len(blocks) - 1, at)
        for b, block in enumerate(blocks):
            pl.when(at == b)(pltpu.make_async_copy(block, held.at[k], in_sems.at[k]).start)
    for k in range(size):
        pltpu.make_async_copy(blocks[0], held.at[k], in_sems.at[k]).wait()
        pltpu.make_async_copy(held.at[k], outs[k], out_sems.at[k]).start()
    for k in range(size):
        pltpu.make_async_copy(held.at[k], outs[k], out_sems.at[k]).wait()


def xor_order(blocks, by, axis):
    size, index = lax.axis_size(axis), lax.axis_index(axis)
    at_end = (index == 0) | (index == size - 1)
    rows, cols = blocks[0].shape
    dtype = blocks[0].dtype
    hbm = pl.BlockSpec(memory_space=pltpu.HBM)
    return pl.pallas_call(
        functools.partial(order_kernel, size),
        in_specs=[pl.BlockSpec(memory_space=pltpu.SMEM)] + [hbm] * len(blocks),
        out_specs=[hbm] * size,
        out_shape=[jax.ShapeDtypeStruct((rows, cols), dtype)] * size,
        scratch_shapes=[pltpu.VMEM((size, rows, cols), dtype), pltpu.SemaphoreType.DMA((size,)), pltpu.SemaphoreType.DMA((size,))],
        cost_estimate=pl.CostEstimate(flops=rows * cols * size, bytes_accessed=4 * rows * cols * size, transcendentals=0),
        name="order",
    )(jnp.stack([by, at_end.astype(jnp.int32)]), *blocks)


def product_kernel(count, *refs):
    lefts, weight = refs[:count], refs[count]
    outs, (left, total) = refs[count + 1 : -2], refs[-2:]
    step = pl.program_id(0)
    at = 0
    for ref in lefts:
        left[at : at + ref.shape[0]] = ref[...]
        at += ref.shape[0]
    term = contract_last(left[...], weight[...])

    @pl.when(step == 0)
    def _():
        total[...] = term

    @pl.when(step > 0)
    def _():
        total[...] += term

    @pl.when(step == pl.num_programs(0) - 1)
    def _():
        for d, out in enumerate(outs):
            n = out.shape[0]
            out[...] = total[d * n : (d + 1) * n].astype(out.dtype)


def product(lefts, weight, dtypes):
    cols, depth = weight.shape
    n = sum(piece.shape[0] for piece in lefts[0])
    rows = n * len(lefts)
    tile = depth // 3 if depth % 768 == 0 and depth > 1536 else depth
    flat = [piece for pieces in lefts for piece in pieces]
    return pl.pallas_call(
        functools.partial(product_kernel, len(flat)),
        grid=(depth // tile,),
        in_specs=[pl.BlockSpec((piece.shape[0], tile), lambda i: (0, i)) for piece in flat] + [pl.BlockSpec((cols, tile), lambda i: (0, i))],
        out_specs=[pl.BlockSpec((n, cols), lambda i: (0, 0))] * len(lefts),
        out_shape=[jax.ShapeDtypeStruct((n, cols), dtype) for dtype in dtypes],
        scratch_shapes=[pltpu.VMEM((rows, tile), weight.dtype), pltpu.VMEM((rows, cols), jnp.float32)],
        cost_estimate=pl.CostEstimate(flops=2 * rows * cols * depth, bytes_accessed=2 * depth * (rows + cols), transcendentals=0),
        name="product",
    )(*flat, weight)


def total_kernel(*refs):
    total = refs[0][...]
    for ref in refs[1:-1]:
        total += ref[...].astype(jnp.float32)
    refs[-1][...] = total.astype(refs[-1].dtype)


def total_of(own, others):
    return pl.pallas_call(
        total_kernel,
        out_shape=jax.ShapeDtypeStruct(own.shape, jnp.bfloat16),
        cost_estimate=pl.CostEstimate(flops=own.size * len(others), bytes_accessed=2 * own.size * (len(others) + 3), transcendentals=0),
        name="total",
    )(own, *others)


def hessian_kernel(toks, subs, more, scaling, sub_ref, *refs):
    out, refs = refs[-1], refs[:-1]
    before, refs = (refs[0], refs[1:]) if more else (None, refs)
    left = jnp.concatenate([ref[...] for ref in refs[:toks]], axis=0)
    cols = left.shape[1]
    for k in range(subs):
        right = jnp.concatenate([ref[...] for ref in refs[toks * (k + 1) : toks * (k + 2)]], axis=0)
        term = contract_rows(left, right) * scaling
        for by in range(subs):

            @pl.when(sub_ref[0] == by)
            def _(k=k, by=by, term=term):
                at = slice((by ^ k) * cols, ((by ^ k) + 1) * cols)
                out[:, at] = term + before[:, at] if more else term


def hessian_of(left, right, scaling, before, sub):
    toks, subs = len(left), len(right)
    n, cols = left[0].shape
    flat = list(left) + [piece for pieces in right for piece in pieces]
    extra = [] if before is None else [before]
    return pl.pallas_call(
        functools.partial(hessian_kernel, toks, subs, len(extra), scaling),
        in_specs=[pl.BlockSpec(memory_space=pltpu.SMEM)] + [pl.BlockSpec(memory_space=pltpu.VMEM)] * (len(flat) + len(extra)),
        out_specs=pl.BlockSpec(memory_space=pltpu.VMEM),
        out_shape=jax.ShapeDtypeStruct((cols, subs * cols), jnp.float32),
        cost_estimate=pl.CostEstimate(flops=2 * toks * n * cols * cols * subs, bytes_accessed=4 * cols * cols * subs, transcendentals=0),
        name="hessian",
    )(sub.reshape(1), *extra, *flat)


def pick_kernel(toks, subs, share, at_ref, *refs):
    outs, sems = refs[-subs - 1 : -1], refs[-1]
    groups, at = [], 0
    count = (len(refs) - subs - 1) // len(GROUPS)
    for g in range(len(GROUPS)):
        blocks = refs[g * count : (g + 1) * count]
        groups.append((at, blocks))
        at += blocks[0].shape[0]
    row, sub, at_end = at_ref[0], at_ref[1], at_ref[2]
    for k in range(subs):
        first = (row * subs + (sub ^ k)) * share
        for q in range(toks):
            b = q ^ row
            b = jnp.where((b == toks - 1) & (at_end == 1), count - 1, b)
            for start, blocks in groups:
                for i, block in enumerate(blocks):

                    @pl.when((b == i) & (first >= start) & (first < start + block.shape[0]))
                    def _(k=k, q=q, block=block, first=first, start=start):
                        rows = block.at[pl.ds(pl.multiple_of(first - start, share), share)]
                        pltpu.make_async_copy(rows, outs[k].at[q], sems.at[k, q]).start()

    for k in range(subs):
        for q in range(toks):
            pltpu.make_async_copy(refs[0].at[pl.ds(0, share)], outs[k].at[q], sems.at[k, q]).wait()


def pick(layer_rows, share, subs):
    toks, row = lax.axis_size("row"), lax.axis_index("row")
    cols = layer_rows[0][0].shape[1]
    flat = [block for blocks in layer_rows for block in blocks]
    at_end = ((row == 0) | (row == toks - 1)).astype(jnp.int32)
    return pl.pallas_call(
        functools.partial(pick_kernel, toks, subs, share),
        in_specs=[pl.BlockSpec(memory_space=pltpu.SMEM)] + [pl.BlockSpec(memory_space=pltpu.HBM)] * len(flat),
        out_specs=[pl.BlockSpec(memory_space=pltpu.VMEM)] * subs,
        out_shape=[jax.ShapeDtypeStruct((toks, share, cols), flat[0].dtype)] * subs,
        scratch_shapes=[pltpu.SemaphoreType.DMA((subs, toks))],
        cost_estimate=pl.CostEstimate(flops=0, bytes_accessed=4 * subs * toks * share * cols, transcendentals=0),
        name="pick",
    )(jnp.stack([row, lax.axis_index("sub"), at_end]), *flat)


def select_order(blocks, by):
    size = len(blocks)
    bit = 1
    while bit < size:
        flip = jnp.broadcast_to((by & bit) != 0, blocks[0].shape)
        blocks = [lax.select(flip, blocks[k ^ bit], blocks[k]) for k in range(size)]
        bit *= 2
    return blocks


def turn(blocks, axis):
    return list(blocks[:1]) + [swap(blocks[k], axis, k) for k in range(1, len(blocks))]


def contract_last(left, right):
    return lax.dot_general(left, right, (((1,), (1,)), ((), ())), preferred_element_type=jnp.float32)


def contract_rows(left, right):
    return lax.dot_general(left, right, (((0,), (0,)), ((), ())), preferred_element_type=jnp.float32)


def body(hidden_in, down_weight, keep_mask):
    tok, row, sub = lax.axis_index("tok"), lax.axis_index("row"), lax.axis_index("sub")
    toks, subs = lax.axis_size("tok"), lax.axis_size("sub")
    rows, depth = hidden_in.shape
    cols = down_weight.shape[0]
    small = jnp.bfloat16
    steps = [rows * share // sum(SHARES) for share in SHARES]
    starts = [sum(steps[:j]) for j in range(len(steps))]

    def pruned(weight, mask, block):
        w = lax.dynamic_slice(weight, (0, block * depth), (cols, depth))
        return w * lax.dynamic_slice(mask, (0, block * depth), (cols, depth)).astype(w.dtype)

    pieces = lax.optimization_barrier([hidden_in[at : at + n] for at, n in zip(starts, steps)])
    seen = [spread_first(piece, "row") for piece in pieces]

    sent = [swap(pruned(down_weight, keep_mask, sub ^ k), "sub", k) for k in range(1, subs)]
    weight, mask, _ = lax.optimization_barrier((down_weight, keep_mask, seen[0][1]))
    weights = [pruned(weight, mask, sub)] + sent

    arrived = []
    for j in range(len(steps)):
        blocks = spread_last(seen[j], "row")
        arrived.append(turn(xor_order(blocks, tok ^ row, "row"), "tok"))

    def across(value, d, k):
        pairs = [(t * subs + s, (t ^ d) * subs + (s ^ k)) for t in range(toks) for s in range(subs)]
        return lax.ppermute(value, ("tok", "sub"), pairs) if d or k else value

    hessian, layer_rows = None, []
    scaling = 2.0 / (rows * toks)
    for group in GROUPS:
        lefts = [[arrived[j][d] for j in group] for d in range(toks)]
        terms = [product(lefts, weights[k], [small if k or d else jnp.float32 for d in range(toks)]) for k in range(subs)]
        others = [across(terms[k][d], d, k) for k in reversed(range(subs)) for d in range(toks) if d or k]
        layer = total_of(terms[0][0], others)
        blocks = spread(layer, "row")
        layer_rows.append(blocks)
        mine = xor_order(blocks, tok ^ row, "row")
        left = turn([layer] * toks, "tok")
        right = [[across(mine[d], d, k) for d in range(toks)] for k in range(subs)]
        hessian = hessian_of(left, right, scaling, hessian, sub)

    share = rows // (toks * subs)
    pieces = pick(layer_rows, share, subs)
    pieces = list(pieces[:1]) + [swap(pieces[k], "sub", k) for k in range(1, subs)]
    layer_out = jnp.stack(select_order(pieces, sub), axis=1).transpose(2, 0, 1, 3).reshape(share, toks * subs * cols)
    return layer_out, hessian


def solution(mesh):
    toks, both = mesh.shape["tok"], mesh.shape["col"]
    subs = both // toks
    grid = Mesh(mesh.devices.reshape(toks, toks, subs), ("tok", "row", "sub"))
    col = ("row", "sub")
    in_specs = (P("tok", col), P(col, "tok"), P(col, "tok"))
    out_specs = (P(("tok",) + col, None), P(col, "tok"))
    return jax.shard_map(body, mesh=grid, in_specs=in_specs, out_specs=out_specs, check_vma=False)
```

```python
import functools
import math

import jax
import jax.numpy as jnp
from jax import lax
from jax.experimental import pallas as pl
from jax.experimental.pallas import tpu as pltpu
from jax.sharding import Mesh, PartitionSpec as P


SHARES = (4, 4, 4, 2, 2)
GROUPS = ((0, 1, 2), (3, 4))


def swap(value, axis, offset):
    return lax.ppermute(value, axis, [(i, i ^ offset) for i in range(lax.axis_size(axis))])


def spread_first(value, axis):
    size = lax.axis_size(axis)
    if size != 4:
        return [value] + [swap(value, axis, k) for k in range(1, size)]
    middle = lax.ppermute(value, axis, [(1, 2), (2, 1)])
    far = lax.ppermute(value, axis, [(0, 2), (3, 1)])
    return [value, lax.ppermute(value, axis, [(i, i ^ 1) for i in range(size)]), far, middle]


def spread_last(blocks, axis):
    if lax.axis_size(axis) != 4:
        return blocks
    ends = [(1, 0), (2, 3)]
    return list(blocks) + [lax.ppermute(blocks[3], axis, ends), lax.ppermute(blocks[2], axis, ends)]


def spread_small(value, axis):
    size = lax.axis_size(axis)
    near, *rest = [swap(value, axis, k) for k in range(1, size if size != 4 else 3)]
    if size != 4:
        return [value, near] + rest
    middle = lax.ppermute(value, axis, [(1, 2), (2, 1)])
    return [value, near] + rest + [middle, lax.ppermute(rest[0], axis, [(1, 0), (2, 3)])]


def place(at, size, count, at_end):
    return jnp.where((at >= 2 * size - count) & (at_end == 1), at + count - size, at)


def order_kernel(size, by_ref, *refs):
    outs, (held, in_sems, out_sems) = refs[-size - 3 : -3], refs[-3:]
    blocks = refs[: -size - 3]
    for k in range(size):
        at = k ^ by_ref[0]
        at = place(at, size, len(blocks), by_ref[1])
        for b, block in enumerate(blocks):
            pl.when(at == b)(pltpu.make_async_copy(block, held.at[k], in_sems.at[k]).start)
    for k in range(size):
        pltpu.make_async_copy(blocks[0], held.at[k], in_sems.at[k]).wait()
        pltpu.make_async_copy(held.at[k], outs[k], out_sems.at[k]).start()
    for k in range(size):
        pltpu.make_async_copy(held.at[k], outs[k], out_sems.at[k]).wait()


def xor_order(blocks, by, axis):
    size, index = lax.axis_size(axis), lax.axis_index(axis)
    at_end = (index == 0) | (index == size - 1)
    rows, cols = blocks[0].shape
    dtype = blocks[0].dtype
    hbm = pl.BlockSpec(memory_space=pltpu.HBM)
    return pl.pallas_call(
        functools.partial(order_kernel, size),
        in_specs=[pl.BlockSpec(memory_space=pltpu.SMEM)] + [hbm] * len(blocks),
        out_specs=[hbm] * size,
        out_shape=[jax.ShapeDtypeStruct((rows, cols), dtype)] * size,
        scratch_shapes=[pltpu.VMEM((size, rows, cols), dtype), pltpu.SemaphoreType.DMA((size,)), pltpu.SemaphoreType.DMA((size,))],
        cost_estimate=pl.CostEstimate(flops=rows * cols * size, bytes_accessed=4 * rows * cols * size, transcendentals=0),
        name="order",
    )(jnp.stack([by, at_end.astype(jnp.int32)]), *blocks)


def product_kernel(count, subs, *refs):
    lefts, weights = refs[:count], refs[count : count + subs]
    keep, send, left, right, total = refs[count + subs :]
    step, toks = pl.program_id(0), 2 * keep.shape[1]
    n, cols = keep.shape[2:]
    at = 0
    for ref in lefts:
        left[at : at + ref.shape[0]] = ref[...]
        at += ref.shape[0]
    for k in range(subs):
        right[k * cols : (k + 1) * cols] = weights[k][...]
    term = contract_last(left[...], right[...])

    @pl.when(step == 0)
    def _():
        total[...] = term

    @pl.when(step > 0)
    def _():
        total[...] += term

    @pl.when(step == pl.num_programs(0) - 1)
    def _():
        for k in range(subs):
            for d in range(0, toks, 2):
                here = slice(k * cols, (k + 1) * cols)
                keep[k, d // 2] = total[d * n : (d + 1) * n, here]
                send[k, d // 2] = total[(d + 1) * n : (d + 2) * n, here].astype(send.dtype)


def product(lefts, weights):
    subs, toks = len(weights), len(lefts)
    cols, depth = weights[0].shape
    n = sum(piece.shape[0] for piece in lefts[0])
    rows = n * toks
    parts = 2 if rows <= 512 else 3
    tile = depth // parts if depth % (parts * 128) == 0 and depth > 2048 else depth
    flat = [piece for pieces in lefts for piece in pieces]
    shape = (subs, toks // 2, n, cols)
    return pl.pallas_call(
        functools.partial(product_kernel, len(flat), subs),
        grid=(depth // tile,),
        in_specs=[pl.BlockSpec((piece.shape[0], tile), lambda i: (0, i)) for piece in flat]
        + [pl.BlockSpec((cols, tile), lambda i: (0, i))] * subs,
        out_specs=[pl.BlockSpec(shape, lambda i: (0, 0, 0, 0))] * 2,
        out_shape=[jax.ShapeDtypeStruct(shape, jnp.float32), jax.ShapeDtypeStruct(shape, jnp.bfloat16)],
        scratch_shapes=[
            pltpu.VMEM((rows, tile), jnp.bfloat16),
            pltpu.VMEM((subs * cols, tile), jnp.bfloat16),
            pltpu.VMEM((rows, subs * cols), jnp.float32),
        ],
        cost_estimate=pl.CostEstimate(
            flops=2 * rows * cols * depth * subs, bytes_accessed=2 * depth * (rows + cols * subs), transcendentals=0
        ),
        name="product",
    )(*flat, *weights)


def pair_kernel(keep, arrived, *outs):
    half = keep.shape[1]
    for i, out in enumerate(outs):
        out[...] = (keep[i // half, i % half] + arrived[i // half, i % half].astype(jnp.float32)).astype(out.dtype)


def pair(keep, arrived):
    subs, half, n, cols = keep.shape
    outs = pl.pallas_call(
        pair_kernel,
        out_shape=[jax.ShapeDtypeStruct((n, cols), jnp.bfloat16 if i else jnp.float32) for i in range(subs * half)],
        cost_estimate=pl.CostEstimate(flops=keep.size, bytes_accessed=8 * keep.size, transcendentals=0),
        name="pair",
    )(keep, arrived)
    return [outs[k * half : (k + 1) * half] for k in range(subs)]


def total_kernel(*refs):
    total = refs[0][...]
    for ref in refs[1:-1]:
        total += ref[...].astype(jnp.float32)
    refs[-1][...] = total.astype(refs[-1].dtype)


def total_of(own, others):
    return pl.pallas_call(
        total_kernel,
        out_shape=jax.ShapeDtypeStruct(own.shape, jnp.bfloat16),
        cost_estimate=pl.CostEstimate(flops=own.size * len(others), bytes_accessed=2 * own.size * (len(others) + 3), transcendentals=0),
        name="total",
    )(own, *others)


def hessian_kernel(pieces, subs, scaling, sub_ref, *refs):
    out, refs = refs[-1], refs[:-1]

    def stacked(k):
        return jnp.concatenate([ref[...] for ref in refs[k * pieces : (k + 1) * pieces]], axis=0)

    left = stacked(0)
    cols = left.shape[1]
    for k in range(subs):
        term = contract_rows(left, stacked(k + 1)) * scaling
        for by in range(subs):

            @pl.when(sub_ref[0] == by)
            def _(k=k, by=by, term=term):
                out[:, (by ^ k) * cols : ((by ^ k) + 1) * cols] = term


def hessian_of(left, right, scaling, sub):
    subs, cols = len(right), left[0].shape[1]
    rows = sum(piece.shape[0] for piece in left)
    vmem = pl.BlockSpec(memory_space=pltpu.VMEM)
    return pl.pallas_call(
        functools.partial(hessian_kernel, len(left), subs, scaling),
        in_specs=[pl.BlockSpec(memory_space=pltpu.SMEM)] + [vmem] * (len(left) * (subs + 1)),
        out_specs=vmem,
        out_shape=jax.ShapeDtypeStruct((cols, subs * cols), jnp.float32),
        cost_estimate=pl.CostEstimate(flops=2 * rows * cols * cols * subs, bytes_accessed=4 * cols * cols * subs, transcendentals=0),
        name="hessian",
    )(sub.reshape(1), *left, *[piece for pieces in right for piece in pieces])


def pick_kernel(toks, subs, share, at_ref, *refs):
    outs, sems = refs[-subs - 1 : -1], refs[-1]
    groups, at = [], 0
    count = (len(refs) - subs - 1) // len(GROUPS)
    for g in range(len(GROUPS)):
        blocks = refs[g * count : (g + 1) * count]
        groups.append((at, blocks))
        at += blocks[0].shape[0]
    row, sub, at_end = at_ref[0], at_ref[1], at_ref[2]
    grain = math.gcd(share, *[blocks[0].shape[0] for _, blocks in groups])
    for k in range(subs):
        for q in range(toks):
            b = place(q ^ row, toks, count, at_end)
            for piece in range(0, share, grain):
                first = (row * subs + (sub ^ k)) * share + piece
                for start, blocks in groups:
                    for i, block in enumerate(blocks):

                        @pl.when((b == i) & (first >= start) & (first < start + block.shape[0]))
                        def _(k=k, q=q, block=block, first=first, start=start, piece=piece):
                            rows = block.at[pl.ds(pl.multiple_of(first - start, grain), grain)]
                            pltpu.make_async_copy(rows, outs[k].at[q, pl.ds(piece, grain)], sems.at[k, q]).start()

    for k in range(subs):
        for q in range(toks):
            pltpu.make_async_copy(refs[0].at[pl.ds(0, share)], outs[k].at[q], sems.at[k, q]).wait()


def pick(layer_rows, share, subs):
    toks, row = lax.axis_size("row"), lax.axis_index("row")
    cols = layer_rows[0][0].shape[1]
    flat = [block for blocks in layer_rows for block in blocks]
    at_end = ((row == 0) | (row == toks - 1)).astype(jnp.int32)
    return pl.pallas_call(
        functools.partial(pick_kernel, toks, subs, share),
        in_specs=[pl.BlockSpec(memory_space=pltpu.SMEM)] + [pl.BlockSpec(memory_space=pltpu.HBM)] * len(flat),
        out_specs=[pl.BlockSpec(memory_space=pltpu.VMEM)] * subs,
        out_shape=[jax.ShapeDtypeStruct((toks, share, cols), flat[0].dtype)] * subs,
        scratch_shapes=[pltpu.SemaphoreType.DMA((subs, toks))],
        cost_estimate=pl.CostEstimate(flops=0, bytes_accessed=4 * subs * toks * share * cols, transcendentals=0),
        name="pick",
    )(jnp.stack([row, lax.axis_index("sub"), at_end]), *flat)


def select_order(blocks, by):
    size = len(blocks)
    bit = 1
    while bit < size:
        flip = jnp.broadcast_to((by & bit) != 0, blocks[0].shape)
        blocks = [lax.select(flip, blocks[k ^ bit], blocks[k]) for k in range(size)]
        bit *= 2
    return blocks


def turn(blocks, axis):
    return list(blocks[:1]) + [swap(blocks[k], axis, k) for k in range(1, len(blocks))]


def contract_last(left, right):
    return lax.dot_general(left, right, (((1,), (1,)), ((), ())), preferred_element_type=jnp.float32)


def contract_rows(left, right):
    return lax.dot_general(left, right, (((0,), (0,)), ((), ())), preferred_element_type=jnp.float32)


def body(hidden_in, down_weight, keep_mask):
    tok, row, sub = lax.axis_index("tok"), lax.axis_index("row"), lax.axis_index("sub")
    toks, subs = lax.axis_size("tok"), lax.axis_size("sub")
    rows, depth = hidden_in.shape
    cols = down_weight.shape[0]
    steps = [rows * share // sum(SHARES) for share in SHARES]
    starts = [sum(steps[:j]) for j in range(len(steps))]

    def pruned(weight, mask, block):
        w = lax.dynamic_slice(weight, (0, block * depth), (cols, depth))
        return w * lax.dynamic_slice(mask, (0, block * depth), (cols, depth)).astype(w.dtype)

    pieces = [lax.optimization_barrier(hidden_in[at : at + n]) for at, n in zip(starts, steps)]
    seen = [spread_first(piece, "row") for piece in pieces]

    sent = [swap(pruned(down_weight, keep_mask, sub ^ k), "sub", k) for k in range(1, subs)]
    weight, mask, _ = lax.optimization_barrier((down_weight, keep_mask, seen[0][1]))
    kept, second = lax.optimization_barrier((pruned(weight, mask, sub), seen[1][2]))
    seen[1][2] = second
    weights = [kept] + sent

    arrived = []
    for j in range(len(steps)):
        blocks = spread_last(seen[j], "row")
        blocks = xor_order(blocks, tok ^ row, "row")
        arrived.append(turn(blocks, "tok"))

    def across(value, d, k):
        pairs = [(t * subs + s, (t ^ d) * subs + (s ^ k)) for t in range(toks) for s in range(subs)]
        return lax.ppermute(value, ("tok", "sub"), pairs) if d or k else value

    left, right, layer_rows = [], [[] for _ in range(subs)], []
    scaling = 2.0 / (rows * toks)
    for group in GROUPS:
        lefts = [[arrived[j][d] for j in group] for d in range(toks)]
        keep, send = product(lefts, weights)
        send = swap(send, "tok", 1)
        terms = pair(keep, send)
        others = [across(terms[k][d // 2], d, k) for k in range(subs) for d in range(0, toks, 2) if d or k]
        layer = total_of(terms[0][0], others)
        blocks = spread_small(layer, "row")
        layer_rows.append(blocks)
        mine = xor_order(blocks, tok ^ row, "row")
        left += turn([layer] * toks, "tok")
        for k in range(subs):
            right[k] += [across(mine[d], d, k) for d in range(toks)]
    hessian = hessian_of(left, right, scaling, sub)

    share = rows // (toks * subs)
    pieces = pick(layer_rows, share, subs)
    pieces = list(pieces[:1]) + [swap(pieces[k], "sub", k) for k in range(1, subs)]
    layer_out = jnp.stack(select_order(pieces, sub), axis=1).transpose(2, 0, 1, 3).reshape(share, toks * subs * cols)
    return layer_out, hessian


def solution(mesh):
    toks, both = mesh.shape["tok"], mesh.shape["col"]
    subs = both // toks
    grid = Mesh(mesh.devices.reshape(toks, toks, subs), ("tok", "row", "sub"))
    col = ("row", "sub")
    in_specs = (P("tok", col), P(col, "tok"), P(col, "tok"))
    out_specs = (P(("tok",) + col, None), P(col, "tok"))
    return jax.shard_map(body, mesh=grid, in_specs=in_specs, out_specs=out_specs, check_vma=False)
```

```python
import functools
import math

import jax
import jax.numpy as jnp
from jax import lax
from jax.experimental import pallas as pl
from jax.experimental.pallas import tpu as pltpu
from jax.sharding import Mesh, PartitionSpec as P


SHARES = (4, 4, 2, 4, 2)
GROUPS = ((0, 1, 2), (3, 4))


def swap(value, axis, offset):
    return lax.ppermute(value, axis, [(i, i ^ offset) for i in range(lax.axis_size(axis))])


def spread_first(value, axis):
    size = lax.axis_size(axis)
    if size != 4:
        return [value] + [swap(value, axis, k) for k in range(1, size)]
    middle = lax.ppermute(value, axis, [(1, 2), (2, 1)])
    far = lax.ppermute(value, axis, [(0, 2), (3, 1)])
    return [value, lax.ppermute(value, axis, [(i, i ^ 1) for i in range(size)]), far, middle]


def spread_last(blocks, axis):
    if lax.axis_size(axis) != 4:
        return blocks
    ends = [(1, 0), (2, 3)]
    return list(blocks) + [lax.ppermute(blocks[3], axis, ends), lax.ppermute(blocks[2], axis, ends)]


def spread_small(value, axis):
    size = lax.axis_size(axis)
    near, *rest = [swap(value, axis, k) for k in range(1, size if size != 4 else 3)]
    if size != 4:
        return [value, near] + rest
    middle = lax.ppermute(value, axis, [(1, 2), (2, 1)])
    return [value, near] + rest + [middle, lax.ppermute(rest[0], axis, [(1, 0), (2, 3)])]


def place(at, size, count, at_end):
    return jnp.where((at >= 2 * size - count) & (at_end == 1), at + count - size, at)


def order_kernel(size, by_ref, *refs):
    outs, (held, in_sems, out_sems) = refs[-size - 3 : -3], refs[-3:]
    blocks = refs[: -size - 3]
    for k in range(size):
        at = k ^ by_ref[0]
        at = place(at, size, len(blocks), by_ref[1])
        for b, block in enumerate(blocks):
            pl.when(at == b)(pltpu.make_async_copy(block, held.at[k], in_sems.at[k]).start)
    for k in range(size):
        pltpu.make_async_copy(blocks[0], held.at[k], in_sems.at[k]).wait()
        pltpu.make_async_copy(held.at[k], outs[k], out_sems.at[k]).start()
    for k in range(size):
        pltpu.make_async_copy(held.at[k], outs[k], out_sems.at[k]).wait()


def xor_order(blocks, by, axis):
    size, index = lax.axis_size(axis), lax.axis_index(axis)
    at_end = (index == 0) | (index == size - 1)
    rows, cols = blocks[0].shape
    dtype = blocks[0].dtype
    hbm = pl.BlockSpec(memory_space=pltpu.HBM)
    return pl.pallas_call(
        functools.partial(order_kernel, size),
        in_specs=[pl.BlockSpec(memory_space=pltpu.SMEM)] + [hbm] * len(blocks),
        out_specs=[hbm] * size,
        out_shape=[jax.ShapeDtypeStruct((rows, cols), dtype)] * size,
        scratch_shapes=[pltpu.VMEM((size, rows, cols), dtype), pltpu.SemaphoreType.DMA((size,)), pltpu.SemaphoreType.DMA((size,))],
        cost_estimate=pl.CostEstimate(flops=rows * cols * size, bytes_accessed=4 * rows * cols * size, transcendentals=0),
        name="order",
    )(jnp.stack([by, at_end.astype(jnp.int32)]), *blocks)


def product_kernel(count, subs, *refs):
    lefts, weights = refs[:count], refs[count : count + subs]
    keep, send, left, right, total = refs[count + subs :]
    step, toks = pl.program_id(0), 2 * keep.shape[1]
    n, cols = keep.shape[2:]
    at = 0
    for ref in lefts:
        left[at : at + ref.shape[0]] = ref[...]
        at += ref.shape[0]
    for k in range(subs):
        right[k * cols : (k + 1) * cols] = weights[k][...]
    term = contract_last(left[...], right[...])

    @pl.when(step == 0)
    def _():
        total[...] = term

    @pl.when(step > 0)
    def _():
        total[...] += term

    @pl.when(step == pl.num_programs(0) - 1)
    def _():
        for k in range(subs):
            for d in range(0, toks, 2):
                here = slice(k * cols, (k + 1) * cols)
                keep[k, d // 2] = total[d * n : (d + 1) * n, here]
                send[k, d // 2] = total[(d + 1) * n : (d + 2) * n, here].astype(send.dtype)


def product(lefts, weights):
    subs, toks = len(weights), len(lefts)
    cols, depth = weights[0].shape
    n = sum(piece.shape[0] for piece in lefts[0])
    rows = n * toks
    parts = 2 if rows <= 512 else 3
    tile = depth // parts if depth % (parts * 128) == 0 and depth > 2048 else depth
    flat = [piece for pieces in lefts for piece in pieces]
    shape = (subs, toks // 2, n, cols)
    return pl.pallas_call(
        functools.partial(product_kernel, len(flat), subs),
        grid=(depth // tile,),
        in_specs=[pl.BlockSpec((piece.shape[0], tile), lambda i: (0, i)) for piece in flat]
        + [pl.BlockSpec((cols, tile), lambda i: (0, i))] * subs,
        out_specs=[pl.BlockSpec(shape, lambda i: (0, 0, 0, 0))] * 2,
        out_shape=[jax.ShapeDtypeStruct(shape, jnp.float32), jax.ShapeDtypeStruct(shape, jnp.bfloat16)],
        scratch_shapes=[
            pltpu.VMEM((rows, tile), jnp.bfloat16),
            pltpu.VMEM((subs * cols, tile), jnp.bfloat16),
            pltpu.VMEM((rows, subs * cols), jnp.float32),
        ],
        cost_estimate=pl.CostEstimate(
            flops=2 * rows * cols * depth * subs, bytes_accessed=2 * depth * (rows + cols * subs), transcendentals=0
        ),
        name="product",
    )(*flat, *weights)


def pair_kernel(keep, arrived, *outs):
    half = keep.shape[1]
    for i, out in enumerate(outs):
        out[...] = (keep[i // half, i % half] + arrived[i // half, i % half].astype(jnp.float32)).astype(out.dtype)


def pair(keep, arrived):
    subs, half, n, cols = keep.shape
    outs = pl.pallas_call(
        pair_kernel,
        out_shape=[jax.ShapeDtypeStruct((n, cols), jnp.bfloat16 if i else jnp.float32) for i in range(subs * half)],
        cost_estimate=pl.CostEstimate(flops=keep.size, bytes_accessed=8 * keep.size, transcendentals=0),
        name="pair",
    )(keep, arrived)
    return [outs[k * half : (k + 1) * half] for k in range(subs)]


def total_kernel(*refs):
    total = refs[0][...]
    for ref in refs[1:-1]:
        total += ref[...].astype(jnp.float32)
    refs[-1][...] = total.astype(refs[-1].dtype)


def total_of(own, others):
    return pl.pallas_call(
        total_kernel,
        out_shape=jax.ShapeDtypeStruct(own.shape, jnp.bfloat16),
        cost_estimate=pl.CostEstimate(flops=own.size * len(others), bytes_accessed=2 * own.size * (len(others) + 3), transcendentals=0),
        name="total",
    )(own, *others)


def hessian_kernel(pieces, subs, scaling, sub_ref, *refs):
    out, refs = refs[-1], refs[:-1]

    def stacked(k):
        return jnp.concatenate([ref[...] for ref in refs[k * pieces : (k + 1) * pieces]], axis=0)

    left = stacked(0)
    cols = left.shape[1]
    for k in range(subs):
        term = contract_rows(left, stacked(k + 1)) * scaling
        for by in range(subs):

            @pl.when(sub_ref[0] == by)
            def _(k=k, by=by, term=term):
                out[:, (by ^ k) * cols : ((by ^ k) + 1) * cols] = term


def hessian_of(left, right, scaling, sub):
    subs, cols = len(right), left[0].shape[1]
    rows = sum(piece.shape[0] for piece in left)
    vmem = pl.BlockSpec(memory_space=pltpu.VMEM)
    return pl.pallas_call(
        functools.partial(hessian_kernel, len(left), subs, scaling),
        in_specs=[pl.BlockSpec(memory_space=pltpu.SMEM)] + [vmem] * (len(left) * (subs + 1)),
        out_specs=vmem,
        out_shape=jax.ShapeDtypeStruct((cols, subs * cols), jnp.float32),
        cost_estimate=pl.CostEstimate(flops=2 * rows * cols * cols * subs, bytes_accessed=4 * cols * cols * subs, transcendentals=0),
        name="hessian",
    )(sub.reshape(1), *left, *[piece for pieces in right for piece in pieces])


def pick_kernel(toks, subs, share, at_ref, *refs):
    outs, sems = refs[-subs - 1 : -1], refs[-1]
    groups, at = [], 0
    count = (len(refs) - subs - 1) // len(GROUPS)
    for g in range(len(GROUPS)):
        blocks = refs[g * count : (g + 1) * count]
        groups.append((at, blocks))
        at += blocks[0].shape[0]
    row, sub, at_end = at_ref[0], at_ref[1], at_ref[2]
    grain = math.gcd(share, *[blocks[0].shape[0] for _, blocks in groups])
    for k in range(subs):
        for q in range(toks):
            b = place(q ^ row, toks, count, at_end)
            for piece in range(0, share, grain):
                first = (row * subs + (sub ^ k)) * share + piece
                for start, blocks in groups:
                    for i, block in enumerate(blocks):

                        @pl.when((b == i) & (first >= start) & (first < start + block.shape[0]))
                        def _(k=k, q=q, block=block, first=first, start=start, piece=piece):
                            rows = block.at[pl.ds(pl.multiple_of(first - start, grain), grain)]
                            pltpu.make_async_copy(rows, outs[k].at[q, pl.ds(piece, grain)], sems.at[k, q]).start()

    for k in range(subs):
        for q in range(toks):
            pltpu.make_async_copy(refs[0].at[pl.ds(0, share)], outs[k].at[q], sems.at[k, q]).wait()


def pick(layer_rows, share, subs):
    toks, row = lax.axis_size("row"), lax.axis_index("row")
    cols = layer_rows[0][0].shape[1]
    flat = [block for blocks in layer_rows for block in blocks]
    at_end = ((row == 0) | (row == toks - 1)).astype(jnp.int32)
    return pl.pallas_call(
        functools.partial(pick_kernel, toks, subs, share),
        in_specs=[pl.BlockSpec(memory_space=pltpu.SMEM)] + [pl.BlockSpec(memory_space=pltpu.HBM)] * len(flat),
        out_specs=[pl.BlockSpec(memory_space=pltpu.VMEM)] * subs,
        out_shape=[jax.ShapeDtypeStruct((toks, share, cols), flat[0].dtype)] * subs,
        scratch_shapes=[pltpu.SemaphoreType.DMA((subs, toks))],
        cost_estimate=pl.CostEstimate(flops=0, bytes_accessed=4 * subs * toks * share * cols, transcendentals=0),
        name="pick",
    )(jnp.stack([row, lax.axis_index("sub"), at_end]), *flat)


def select_order(blocks, by):
    size = len(blocks)
    bit = 1
    while bit < size:
        flip = jnp.broadcast_to((by & bit) != 0, blocks[0].shape)
        blocks = [lax.select(flip, blocks[k ^ bit], blocks[k]) for k in range(size)]
        bit *= 2
    return blocks


def turn(blocks, axis):
    return list(blocks[:1]) + [swap(blocks[k], axis, k) for k in range(1, len(blocks))]


def contract_last(left, right):
    return lax.dot_general(left, right, (((1,), (1,)), ((), ())), preferred_element_type=jnp.float32)


def contract_rows(left, right):
    return lax.dot_general(left, right, (((0,), (0,)), ((), ())), preferred_element_type=jnp.float32)


def body(hidden_in, down_weight, keep_mask):
    tok, row, sub = lax.axis_index("tok"), lax.axis_index("row"), lax.axis_index("sub")
    toks, subs = lax.axis_size("tok"), lax.axis_size("sub")
    rows, depth = hidden_in.shape
    cols = down_weight.shape[0]
    steps = [rows * share // sum(SHARES) for share in SHARES]
    starts = [sum(steps[:j]) for j in range(len(steps))]

    def pruned(weight, mask, block):
        w = lax.dynamic_slice(weight, (0, block * depth), (cols, depth))
        return w * lax.dynamic_slice(mask, (0, block * depth), (cols, depth)).astype(w.dtype)

    pieces = [lax.optimization_barrier(hidden_in[at : at + n]) for at, n in zip(starts, steps)]
    seen = [spread_first(piece, "row") for piece in pieces]

    sent = [swap(pruned(down_weight, keep_mask, sub ^ k), "sub", k) for k in range(1, subs)]
    weight, mask, _ = lax.optimization_barrier((down_weight, keep_mask, seen[0][1]))
    weights = [pruned(weight, mask, sub)] + sent

    arrived = []
    for j in range(len(steps)):
        blocks = spread_last(seen[j], "row")
        blocks = xor_order(blocks, tok ^ row, "row")
        arrived.append(turn(blocks, "tok"))

    def across(value, d, k):
        pairs = [(t * subs + s, (t ^ d) * subs + (s ^ k)) for t in range(toks) for s in range(subs)]
        return lax.ppermute(value, ("tok", "sub"), pairs) if d or k else value

    left, right, layer_rows = [], [[] for _ in range(subs)], []
    scaling = 2.0 / (rows * toks)
    for group in GROUPS:
        lefts = [[arrived[j][d] for j in group] for d in range(toks)]
        keep, send = product(lefts, weights)
        send = swap(send, "tok", 1)
        terms = pair(keep, send)
        others = [across(terms[k][d // 2], d, k) for k in range(subs) for d in range(0, toks, 2) if d or k]
        layer = total_of(terms[0][0], others)
        blocks = spread_small(layer, "row")
        layer_rows.append(blocks)
        mine = xor_order(blocks, tok ^ row, "row")
        left += turn([layer] * toks, "tok")
        mine = [across(mine[d], d, 0) for d in range(toks)]
        right[0] += mine
        for k in range(1, subs):
            right[k] += [swap(mine[d], "sub", k) for d in range(toks)]
    hessian = hessian_of(left, right, scaling, sub)

    share = rows // (toks * subs)
    pieces = pick(layer_rows, share, subs)
    pieces = list(pieces[:1]) + [swap(pieces[k], "sub", k) for k in range(1, subs)]
    layer_out = jnp.stack(select_order(pieces, sub), axis=1).transpose(2, 0, 1, 3).reshape(share, toks * subs * cols)
    return layer_out, hessian


def solution(mesh):
    toks, both = mesh.shape["tok"], mesh.shape["col"]
    subs = both // toks
    grid = Mesh(mesh.devices.reshape(toks, toks, subs), ("tok", "row", "sub"))
    col = ("row", "sub")
    in_specs = (P("tok", col), P(col, "tok"), P(col, "tok"))
    out_specs = (P(("tok",) + col, None), P(col, "tok"))
    return jax.shard_map(body, mesh=grid, in_specs=in_specs, out_specs=out_specs, check_vma=False)
```
